32 devices in a mesh: row: 8 (over y, x, core), col: 4 (over z).
Axes of the slice: x: 2, y: 2, z: 4, core: 2. Of those that a mesh axis runs over, the one named last changes fastest.
Arguments:
- homolog_representation: bfloat16 [64, 128, 64], P('row', 'col'), may hold values from -1.5 to 1.5
- pair_state: bfloat16 [128, 128, 128], P('row', 'col'), may hold values from -6 to 6
- homolog_present: int32 [64], replicated, may hold values 0 or 1
- token_live_mask: int32 [128], replicated, may hold values 0 or 1
- product_projection: bfloat16 [64, 64], replicated, may hold values from -0.75 to 0.75
- mean_matrix: bfloat16 [1024, 128], replicated, may hold values from -0.75 to 0.75
- score_matrix: float32 [128, 8], replicated, may hold values from -17.5 to 17.5
- payload_projection: bfloat16 [64, 256], replicated, may hold values from -0.75 to 0.75
- switch_projection: bfloat16 [64, 256], replicated, may hold values from -0.75 to 0.75
- return_projection: bfloat16 [256, 64], replicated, may hold values from -1.5 to 1.5
- transition_input: bfloat16 [128, 1024], replicated, may hold values from -0.5 to 0.5
- transition_output: bfloat16 [512, 128], replicated, may hold values from -0.25 to 0.25
Outputs:
- alignment_output: bfloat16 [64, 128, 64], P('row', 'col')
- pair_output: bfloat16 [128, 128, 128], P('row', 'col')
The draws below stay inside these ranges and needn't reach their ends.
All inputs are finite; a program needn't handle non-finite values.
Results may differ from the reference program's by a relative error of at most 0.038.
Values may be sent and summed in bfloat16 or wider, within the bound.
No kernel may reach another device: no remote copies, remote signals or barrier semaphores. Data moves between devices by JAX's collectives and lax.ppermute only.
A program may use at most 64 MiB of HBM per device.

```python
import jax
import jax.numpy as jnp
from jax import lax

HOMOLOG_FEATURES = 64
CZ = 128
PRODUCT_FEATURES = 32
BLEND_GROUPS = 8
GROUP_FEATURES = 32
FF = 512
TOK_ROW = 16
RESIDUE_SPAN = 128
HOMOLOG_DEPTH = 64


def spread_scales(key, low, high):
    raw = jax.random.uniform(key, (BLEND_GROUPS,), jnp.float32, 0.0, 1.0)
    placed = (raw - jnp.min(raw)) / (jnp.max(raw) - jnp.min(raw) + 1e-06)
    return jnp.exp(jnp.log(low) + placed * (jnp.log(high) - jnp.log(low)))


def draw_score_matrix(key, part):
    first_key = jax.random.fold_in(jax.random.fold_in(key, 17), 0)
    third_key = jax.random.fold_in(jax.random.fold_in(key, 17), 2)
    head_scale = spread_scales(first_key, 0.008, 0.25)
    base_draw = jnp.clip(jax.random.normal(third_key, (CZ, BLEND_GROUPS), jnp.float32), -4.8, 4.8)
    return base_draw * head_scale[None, :]


def plant(entries, rng, smallest, top_value):
    dims = entries.shape
    spot = [jax.random.randint(jax.random.fold_in(rng, axis), (), 0, dims[axis]) for axis in range(len(dims))]
    entries = entries.at[tuple(spot)].set(smallest)
    longest = dims.index(max(dims))
    spot[longest] = (spot[longest] + 1) % dims[longest]
    return entries.at[tuple(spot)].set(top_value)


def steps_of(own_key, dims, pieces, least, largest):
    factor_of, own = 1.0, jax.random.fold_in(own_key, 6)
    for dim, shards_of in pieces:
        heights = jnp.exp(jax.random.uniform(jax.random.fold_in(own, dim), (shards_of,), jnp.float32, least / len(pieces), largest / len(pieces)))
        factor_of = factor_of * jnp.repeat(heights, dims[dim] // shards_of).reshape([-1 if axis == dim else 1 for axis in range(len(dims))])
    return factor_of


def noise(own_key, shape, scale, limit, shards=(), kind=jnp.bfloat16):
    factor_of = steps_of(own_key, shape, shards, -0.22, 0.18) if shards else 1.0
    entries = jax.random.normal(own_key, shape, jnp.float32) * scale * factor_of
    return jnp.minimum(jnp.maximum(entries, -limit), limit).astype(kind)


def setup_inputs(seed: int = 0) -> dict:
    key_of = jax.random.split(jax.random.key(seed), 13)
    return {
        "homolog_representation": noise(key_of[0], (HOMOLOG_DEPTH, RESIDUE_SPAN, HOMOLOG_FEATURES), 0.1, 1.5, ((0, 8), (1, 4))),
        "pair_state": noise(key_of[1], (RESIDUE_SPAN, RESIDUE_SPAN, CZ), 1.0, 6.0, ((0, 8), (1, 4))),
        "homolog_present": plant((jax.random.randint(key_of[2], (HOMOLOG_DEPTH,), 0, 4) < 3).astype(jnp.int32), jax.random.fold_in(key_of[2], 1), 0, 1),
        "token_live_mask": plant((jax.random.randint(key_of[3], (RESIDUE_SPAN,), 0, 8) < 7).astype(jnp.int32), jax.random.fold_in(key_of[3], 1), 0, 1),
        "product_projection": noise(key_of[4], (HOMOLOG_FEATURES, 2 * PRODUCT_FEATURES), HOMOLOG_FEATURES ** -0.5, 0.75),
        "mean_matrix": noise(key_of[5], (PRODUCT_FEATURES * PRODUCT_FEATURES, CZ), 64 ** -0.5, 0.75),
        "score_matrix": draw_score_matrix(jax.random.fold_in(key_of[12], 71), 0),
        "payload_projection": noise(key_of[7], (HOMOLOG_FEATURES, BLEND_GROUPS * GROUP_FEATURES), HOMOLOG_FEATURES ** -0.5, 0.75),
        "switch_projection": noise(key_of[8], (HOMOLOG_FEATURES, BLEND_GROUPS * GROUP_FEATURES), HOMOLOG_FEATURES ** -0.5, 0.75),
        "return_projection": noise(key_of[9], (BLEND_GROUPS * GROUP_FEATURES, HOMOLOG_FEATURES), 16 ** -0.5, 1.5),
        "transition_input": noise(key_of[10], (CZ, 2 * FF), CZ ** -0.5, 0.5),
        "transition_output": noise(key_of[11], (FF, CZ), FF ** -0.5, 0.25),
    }


epsilon = 1e-05

def normalized_rows(source):
    source = source.astype(jnp.float32)
    center = source - lax.optimization_barrier(jnp.mean(source, axis=-1, keepdims=True))
    spread = lax.optimization_barrier(jnp.mean(center * center, axis=-1, keepdims=True))
    return center * lax.rsqrt(spread + epsilon)

def reference(homolog_representation, pair_state, homolog_present, token_live_mask, product_projection, mean_matrix, score_matrix, payload_projection, switch_projection, return_projection, transition_input, transition_output):
    homolog_standardized = normalized_rows(homolog_representation).astype(jnp.bfloat16)
    homolog_reshaped = homolog_standardized.reshape(HOMOLOG_DEPTH * RESIDUE_SPAN, HOMOLOG_FEATURES)
    homolog_embedding = jnp.dot(homolog_reshaped, product_projection, preferred_element_type=jnp.float32).reshape(HOMOLOG_DEPTH, RESIDUE_SPAN, 2 * PRODUCT_FEATURES)
    sequence_live = homolog_present.astype(jnp.float32)
    left_factor = (homolog_embedding[:, :, :PRODUCT_FEATURES] * sequence_live[:, None, None]).astype(jnp.bfloat16)
    right_factor = homolog_embedding[:, :, PRODUCT_FEATURES:].astype(jnp.bfloat16)
    live_count = jnp.sum(sequence_live)
    residue_present = token_live_mask.astype(jnp.float32)
    starts = jnp.arange(RESIDUE_SPAN // TOK_ROW, dtype=jnp.int32) * TOK_ROW

    def pair_block(block_start):
        left_block = lax.dynamic_slice_in_dim(left_factor, block_start, TOK_ROW, 1)
        outer_sum = jnp.einsum('sic,sjd->ijcd', left_block.astype(jnp.float32), right_factor.astype(jnp.float32))
        row_live = lax.dynamic_slice_in_dim(residue_present, block_start, TOK_ROW, 0)
        pair_live = row_live[:, None] * residue_present[None, :]
        mean_scale = pair_live / jnp.maximum(pair_live * live_count, 1.0)
        pair_mean = (outer_sum * mean_scale[:, :, None, None]).astype(jnp.bfloat16).reshape(TOK_ROW * RESIDUE_SPAN, PRODUCT_FEATURES * PRODUCT_FEATURES)
        pair_block_in = lax.dynamic_slice_in_dim(pair_state, block_start, TOK_ROW, 0).reshape(TOK_ROW * RESIDUE_SPAN, CZ)
        pair_mid = (pair_block_in.astype(jnp.float32) + jnp.dot(pair_mean, mean_matrix, preferred_element_type=jnp.float32)).astype(jnp.bfloat16)
        pair_norm = normalized_rows(pair_mid)
        scores = jnp.dot(pair_norm, score_matrix, precision=lax.Precision.HIGHEST, preferred_element_type=jnp.float32)
        hidden_pre = jnp.dot(pair_norm.astype(jnp.bfloat16), transition_input, preferred_element_type=jnp.float32)
        hidden = (jax.nn.silu(hidden_pre[:, :FF]) * hidden_pre[:, FF:]).astype(jnp.bfloat16)
        pair_new = (pair_mid.astype(jnp.float32) + jnp.dot(hidden, transition_output, preferred_element_type=jnp.float32)).astype(jnp.bfloat16)
        return (pair_new.reshape(TOK_ROW, RESIDUE_SPAN, CZ), scores.reshape(TOK_ROW, RESIDUE_SPAN, BLEND_GROUPS))
    pair_output, scores = lax.map(pair_block, starts)
    pair_output = pair_output.reshape(RESIDUE_SPAN, RESIDUE_SPAN, CZ)
    scores = scores.reshape(RESIDUE_SPAN, RESIDUE_SPAN, BLEND_GROUPS)
    row_top = lax.optimization_barrier(jnp.max(scores, axis=1, keepdims=True))
    exp_scores = jnp.exp(scores - row_top)
    blend_coefficients = (exp_scores / lax.optimization_barrier(jnp.sum(exp_scores, axis=1, keepdims=True))).astype(jnp.bfloat16)
    payload_entries = jnp.dot(homolog_reshaped, payload_projection, preferred_element_type=jnp.float32).reshape(HOMOLOG_DEPTH, RESIDUE_SPAN, BLEND_GROUPS * GROUP_FEATURES)
    payload_entries = (payload_entries * residue_present[None, :, None]).astype(jnp.bfloat16).reshape(HOMOLOG_DEPTH, RESIDUE_SPAN, BLEND_GROUPS, GROUP_FEATURES)
    switch_logistic = jax.nn.sigmoid(jnp.dot(homolog_reshaped, switch_projection, preferred_element_type=jnp.float32)).reshape(HOMOLOG_DEPTH, RESIDUE_SPAN, BLEND_GROUPS * GROUP_FEATURES)
    blended_result = jnp.einsum('qfg,rfgn->rqgn', blend_coefficients.astype(jnp.float32), payload_entries.astype(jnp.float32)).reshape(HOMOLOG_DEPTH, RESIDUE_SPAN, BLEND_GROUPS * GROUP_FEATURES)
    switched_blend = (switch_logistic * blended_result).astype(jnp.bfloat16).reshape(HOMOLOG_DEPTH * RESIDUE_SPAN, BLEND_GROUPS * GROUP_FEATURES)
    residue_couple_delta = jnp.dot(switched_blend, return_projection, preferred_element_type=jnp.float32).reshape(HOMOLOG_DEPTH, RESIDUE_SPAN, HOMOLOG_FEATURES)
    alignment_output = (homolog_representation.astype(jnp.float32) + residue_couple_delta).astype(jnp.bfloat16)
    return (alignment_output, pair_output)
```

```python
import functools

import jax
import jax.numpy as jnp
from jax import lax
from jax.experimental import pallas as pl
from jax.experimental.pallas import tpu as pltpu
from jax.sharding import PartitionSpec as P

EPS = 1e-05
F32 = jnp.float32
BF16 = jnp.bfloat16
VMEM_LIMIT = 40 * 1024 * 1024


def normed(v):
    center = v - jnp.mean(v, axis=-1, keepdims=True)
    spread = jnp.mean(center * center, axis=-1, keepdims=True)
    return center * lax.rsqrt(spread + EPS)


def lane_iota(shape):
    return lax.broadcasted_iota(jnp.int32, shape, len(shape) - 1)


def mm(a, b, dims=((1,), (0,)), precision=None):
    return lax.dot_general(a, b, (dims, ((), ())), precision=precision, preferred_element_type=F32)


def project_kernel(*refs, cols, rows, seqs, col_tok, row_tok, width):
    xs = refs[:cols]
    wp_ref, present_ref, live_ref, send_ref, xn_ref, left_scr, right_scr = refs[cols:]
    row = lax.axis_index("row")
    col = lax.axis_index("col")
    block = seqs * col_tok
    per = 128 // width
    wp = wp_ref[...]
    wl = jnp.concatenate([wp[:, :width]] * per, axis=1)
    wr = jnp.concatenate([wp[:, width:]] * per, axis=1)
    for k in range(cols):
        at = lax.rem(col - k + cols, cols)
        x = xs[k][...].astype(F32).reshape(block, xs[k].shape[2])
        xn = normed(x).astype(BF16)
        xn_ref[at] = xn.reshape(xn_ref.shape[1:])
        left_scr[pl.ds(pl.multiple_of(at * block, block), block), :] = mm(xn, wl)
        if k == 0:
            right_scr[...] = mm(xn, wr)
    sub = lax.broadcasted_iota(jnp.int32, (seqs, 128), 0)
    gran = lane_iota((seqs, 128)) // width
    present = jnp.zeros((seqs, 128), F32)
    for s in range(seqs):
        present = jnp.where(sub == s, present_ref[row * seqs + s].astype(F32), present)

    def tile(scr, base, tok, first):
        out = None
        for g in range(per):
            part = scr[pl.ds(base + tok + g, seqs, stride=col_tok), :]
            part = part * live_ref[first + g].astype(F32)
            out = part if out is None else jnp.where(gran == g, part, out)
        return out

    left_tiles = row_tok // per
    right_tiles = col_tok // per
    for r in range(rows):
        for t in range(left_tiles):
            first = r * row_tok + t * per
            base = (first // col_tok) * block
            v = tile(left_scr, base, first % col_tok, first) * present
            send_ref[r, :, t * 128 : (t + 1) * 128] = v.astype(BF16)
    for t in range(right_tiles):
        v = tile(right_scr, 0, t * per, col * col_tok + t * per).astype(BF16)
        for r in range(rows):
            at = (left_tiles + t) * 128
            send_ref[r, :, at : at + 128] = v


def pair_kernel(
    got_ref, pair_ref, present_ref, mean_ref, score_ref, chunk_ref, mid_ref, pn_ref,
    outer_scr, lhs_scr, pair_scr, *, row_tok, col_tok, width, heads,
):
    per = 128 // width
    total = got_ref.shape[0] * got_ref.shape[1]
    got = got_ref[...].reshape(total, got_ref.shape[2])
    left = got[:, : row_tok * width]
    right = got[:, row_tok * width :]
    count = jnp.sum(present_ref[...].astype(F32), axis=1, keepdims=True)
    inv = 1.0 / jnp.maximum(count, 1.0)
    span = row_tok * width
    tiles_j = col_tok // per
    outer = mm(left, right, ((0,), (0,))) * inv
    for jh in range(tiles_j):
        outer_scr[jh * span : (jh + 1) * span, :] = outer[:, jh * 128 : (jh + 1) * 128]
    gran = lane_iota((row_tok, 128)) // width
    for hi in range(width // per):
        for jh in range(tiles_j):
            a = [outer_scr[pl.ds(jh * span + hi * per + lo, row_tok, stride=width), :] for lo in range(per)]
            step = 1
            while step < per:
                odd = (gran // step) % 2 == 1
                b = list(a)
                for lo in range(per):
                    if (lo // step) % 2 == 0:
                        b[lo] = jnp.where(odd, pltpu.roll(a[lo + step], step * width, 1), a[lo])
                        b[lo + step] = jnp.where(odd, a[lo + step], pltpu.roll(a[lo], 128 - step * width, 1))
                a = b
                step *= 2
            for lo in range(per):
                at = (jh * per + lo) * row_tok
                lhs_scr[at : at + row_tok, hi * 128 : (hi + 1) * 128] = a[lo].astype(BF16)
    delta = mm(lhs_scr[...], mean_ref[...])
    pair_scr[...] = pair_ref[...].astype(F32).reshape(pair_scr.shape)
    state = jnp.concatenate(
        [pair_scr[pl.ds(j, row_tok, stride=col_tok), :] for j in range(col_tok)], axis=0
    )
    mid = (state + delta).astype(BF16)
    mid_ref[...] = mid
    pn = normed(mid.astype(F32))
    pn_ref[...] = pn.astype(BF16)
    scores = mm(score_ref[...], pn, ((1,), (1,)), lax.Precision.HIGHEST)
    sub = lax.broadcasted_iota(jnp.int32, (heads, 128), 0)
    lane_gran = lane_iota((heads, 128)) // row_tok
    turn = jnp.bitwise_and(lane_gran - sub, heads - 1)
    tiles = []
    for t in range(col_tok // heads):
        v = scores[:, t * 128 : (t + 1) * 128]
        out = v
        for k in range(1, heads):
            moved = pltpu.roll(pltpu.roll(v, heads - k, 0), row_tok * k, 1)
            out = jnp.where(turn == k, moved, out)
        tiles.append(out)
    by_token = jnp.concatenate(tiles, axis=0)
    top = jnp.max(by_token, axis=0, keepdims=True).astype(BF16)
    shifted = jnp.exp(by_token - top.astype(F32)).astype(BF16)
    tops = jnp.broadcast_to(top, (8, 128))
    for d in range(chunk_ref.shape[0]):
        chunk_ref[d, :col_tok, :] = shifted
        chunk_ref[d, col_tok:, :] = tops


def transition_kernel(
    pn_ref, mid_ref, win_ref, wout_ref, xn_ref, wv_ref, wg_ref, live_ref,
    out_ref, values_ref, gate_ref, out_scr, *, row_tok, col_tok,
):
    ff = wout_ref.shape[0]
    rows = 8 * row_tok
    for b in range(col_tok // 8):
        pre = mm(pn_ref[b * rows : (b + 1) * rows, :], win_ref[...])
        act = pre[:, :ff]
        hidden = (act / (1.0 + jnp.exp(-act)) * pre[:, ff:]).astype(BF16)
        new = mid_ref[b * rows : (b + 1) * rows, :].astype(F32) + mm(hidden, wout_ref[...])
        for t in range(8):
            out_scr[pl.ds(b * 8 + t, row_tok, stride=col_tok), :] = new[t * row_tok : (t + 1) * row_tok, :]
    out_ref[...] = out_scr[...].astype(BF16).reshape(out_ref.shape)
    cols, seqs, _, width = xn_ref.shape
    own = lax.axis_index("col")
    mixed = wv_ref.shape[1]
    for k in range(cols):
        v = mm(xn_ref[k].reshape(seqs * col_tok, width), wv_ref[...]).reshape(seqs, col_tok, mixed)
        live = live_ref[k * col_tok : (k + 1) * col_tok, :].astype(F32)
        values_ref[:, k * col_tok : (k + 1) * col_tok, :] = (v * live[None]).astype(BF16)
    g = mm(xn_ref[own].reshape(seqs * col_tok, width), wg_ref[...])
    gate_ref[...] = 1.0 / (1.0 + jnp.exp(-g))


def blend_kernel(
    got_ref, values_ref, gate_ref, x_ref, wr_ref, out_ref, *, cols, per_col, row_tok, col_tok, heads
):
    own = lax.axis_index("col")
    lanes = []
    for q in range(per_col):
        first = (own * per_col + q) * cols
        tops = [got_ref[first + k, col_tok:, :].astype(F32)[:1] for k in range(cols)]
        top = functools.reduce(jnp.maximum, tops)
        parts = [got_ref[first + k, :col_tok, :].astype(F32) * jnp.exp(tops[k] - top) for k in range(cols)]
        whole = functools.reduce(lambda a, b: a + b, [jnp.sum(p, axis=0, keepdims=True) for p in parts])
        lanes.append(jnp.concatenate(parts, axis=0) / whole)
    weights = jnp.concatenate([jnp.transpose(v) for v in lanes], axis=0).astype(BF16)
    mixed = values_ref.shape[2]
    head_of = lane_iota((row_tok, mixed)) // (mixed // heads)
    seqs = values_ref.shape[0]
    blocks = []
    for s in range(seqs):
        full = mm(weights, values_ref[s])
        for q in range(per_col):
            acc = None
            for h in range(heads):
                at = (q * heads + h) * row_tok
                part = full[at : at + row_tok, :]
                acc = part if acc is None else jnp.where(head_of == h, part, acc)
            blocks.append(acc)
    average = jnp.concatenate(blocks, axis=0)
    gated = (gate_ref[...] * average).astype(BF16)
    delta = mm(gated, wr_ref[...]).reshape(x_ref.shape)
    out_ref[...] = (x_ref[...].astype(F32) + delta).astype(BF16)


def vmem(n):
    return [pl.BlockSpec(memory_space=pltpu.VMEM)] * n


def smem(n):
    return [pl.BlockSpec(memory_space=pltpu.SMEM)] * n


def params():
    return pltpu.CompilerParams(vmem_limit_bytes=VMEM_LIMIT)


def body(x, pair, present, live, wp, mean, score, wv, wg, wr, win, wout):
    cols = lax.axis_size("col")
    rows = lax.axis_size("row")
    seqs, col_tok, feat = x.shape
    row_tok, _, pair_width = pair.shape
    width = wp.shape[1] // 2
    heads = score.shape[1]
    mixed = wv.shape[1]
    per_col = col_tok // row_tok
    assert col_tok % row_tok == 0 and heads * row_tok == 128 and 128 % width == 0
    pairs = row_tok * col_tok
    sds = jax.ShapeDtypeStruct

    xs = [x]
    for k in range(1, cols):
        xs.append(lax.ppermute(x, "col", [(i, (i + k) % cols) for i in range(cols)]))
    packed = (row_tok + col_tok) * width
    send, xn = pl.pallas_call(
        functools.partial(
            project_kernel, cols=cols, rows=rows, seqs=seqs, col_tok=col_tok, row_tok=row_tok, width=width
        ),
        out_shape=(sds((rows, seqs, packed), BF16), sds((cols, seqs, col_tok, feat), BF16)),
        in_specs=vmem(cols + 1) + smem(2),
        out_specs=tuple(vmem(2)),
        scratch_shapes=[
            pltpu.VMEM((cols * seqs * col_tok, 128), F32),
            pltpu.VMEM((seqs * col_tok, 128), F32),
        ],
        compiler_params=params(),
        name="project",
    )(*xs, wp, present, live)
    got = lax.all_to_all(send, "row", 0, 0)

    devices = rows * cols
    chunk_rows = col_tok + 8
    chunk, mid, pn = pl.pallas_call(
        functools.partial(pair_kernel, row_tok=row_tok, col_tok=col_tok, width=width, heads=heads),
        out_shape=(
            sds((devices, chunk_rows, 128), BF16),
            sds((pairs, pair_width), BF16),
            sds((pairs, pair_width), BF16),
        ),
        in_specs=vmem(5),
        out_specs=tuple(vmem(3)),
        scratch_shapes=[
            pltpu.VMEM((row_tok * width * col_tok * width // 128, 128), F32),
            pltpu.VMEM((pairs, width * width), BF16),
            pltpu.VMEM((pairs, pair_width), F32),
        ],
        compiler_params=params(),
        name="pair",
    )(got, pair, present.reshape(1, -1), mean, score.T)
    scores = lax.all_to_all(chunk, ("row", "col"), 0, 0)

    pair_output, values, gate = pl.pallas_call(
        functools.partial(transition_kernel, row_tok=row_tok, col_tok=col_tok),
        out_shape=(
            sds(pair.shape, BF16),
            sds((seqs, cols * col_tok, mixed), BF16),
            sds((seqs * col_tok, mixed), F32),
        ),
        in_specs=vmem(8),
        out_specs=tuple(vmem(3)),
        scratch_shapes=[pltpu.VMEM((pairs, pair_width), F32)],
        compiler_params=params(),
        cost_estimate=pl.CostEstimate(flops=1_000_000_000, bytes_accessed=2_000_000, transcendentals=400_000),
        name="transition",
    )(pn, mid, win, wout, xn, wv, wg, live.reshape(-1, 1))

    alignment = pl.pallas_call(
        functools.partial(
            blend_kernel, cols=cols, per_col=per_col, row_tok=row_tok, col_tok=col_tok, heads=heads
        ),
        out_shape=sds(x.shape, BF16),
        in_specs=vmem(5),
        out_specs=vmem(1)[0],
        compiler_params=params(),
        name="blend",
    )(scores, values, gate, x, wr)
    return alignment, pair_output


def solution(mesh):
    spread = P("row", "col", None)
    return jax.shard_map(
        body,
        mesh=mesh,
        in_specs=(spread, spread) + (P(),) * 10,
        out_specs=(spread, spread),
        check_vma=False,
    )
```

```python
import functools

import jax
import jax.numpy as jnp
from jax import lax
from jax.experimental import pallas as pl
from jax.experimental.pallas import tpu as pltpu
from jax.sharding import PartitionSpec as P

EPS = 1e-05
F32 = jnp.float32
BF16 = jnp.bfloat16
VMEM_LIMIT = 40 * 1024 * 1024


def normed(v):
    center = v - jnp.mean(v, axis=-1, keepdims=True)
    spread = jnp.mean(center * center, axis=-1, keepdims=True)
    return center * lax.rsqrt(spread + EPS)


def lane_iota(shape):
    return lax.broadcasted_iota(jnp.int32, shape, len(shape) - 1)


def mm(a, b, dims=((1,), (0,)), precision=None):
    return lax.dot_general(a, b, (dims, ((), ())), precision=precision, preferred_element_type=F32)


def own_kernel(
    x_ref, wp_ref, wg_ref, present_ref, flags_ref, live_ref,
    xn_ref, left_ref, right_ref, gate_ref, wl_ref, wr_ref, token_ref, seq_ref, inv_ref, *, width,
):
    row = lax.axis_index("row")
    seqs, col_tok, feat = x_ref.shape
    per = 128 // width
    wp = wp_ref[...]
    wl = jnp.concatenate([wp[:, :width]] * per, axis=1)
    wr = jnp.concatenate([wp[:, width:]] * per, axis=1)
    wl_ref[...] = wl
    wr_ref[...] = wr
    xn = normed(x_ref[...].astype(F32).reshape(seqs * col_tok, feat)).astype(BF16)
    xn_ref[...] = xn.reshape(xn_ref.shape)
    left_ref[...] = mm(xn, wl)
    right_ref[...] = mm(xn, wr)
    gate_ref[...] = 1.0 / (1.0 + jnp.exp(-mm(xn, wg_ref[...])))
    sub = lax.broadcasted_iota(jnp.int32, (seqs, 128), 0)
    gran = lane_iota((1, 128)) // width
    present = jnp.zeros((seqs, 128), F32)
    for s in range(seqs):
        present = jnp.where(sub == s, flags_ref[row * seqs + s].astype(F32), present)
    seq_ref[...] = present
    for t in range(token_ref.shape[0]):
        mask = jnp.zeros((1, 128), F32)
        for g in range(per):
            mask = jnp.where(gran == g, live_ref[t * per + g].astype(F32), mask)
        token_ref[t : t + 1, :] = mask
    count = jnp.sum(present_ref[...].astype(F32), axis=1, keepdims=True)
    inv_ref[...] = jnp.broadcast_to(1.0 / jnp.maximum(count, 1.0), inv_ref.shape)


def pack_kernel(*refs, cols, rows, col_tok, row_tok, width):
    xs = refs[: cols - 1]
    (own_ref, own_left_ref, own_right_ref, wl_ref, wr_ref, token_ref, seq_ref,
     send_ref, xn_ref, left_scr, right_scr) = refs[cols - 1 :]
    col = lax.axis_index("col")
    seqs = own_ref.shape[0]
    block = seqs * col_tok
    per = 128 // width
    for k in range(cols):
        at = lax.rem(col - k + cols, cols)
        here = pl.ds(pl.multiple_of(at * block, block), block)
        if k == 0:
            xn_ref[at] = own_ref[...]
            left_scr[here, :] = own_left_ref[...]
            right_scr[here, :] = own_right_ref[...]
        else:
            v = xs[k - 1][...]
            xn = normed(v.astype(F32).reshape(block, v.shape[2])).astype(BF16)
            xn_ref[at] = xn.reshape(xn_ref.shape[1:])
            left_scr[here, :] = mm(xn, wl_ref[...])
            right_scr[here, :] = mm(xn, wr_ref[...])
    gran = lane_iota((seqs, 128)) // width
    present = seq_ref[...]

    def tile(scr, base, tok, mask):
        out = None
        for g in range(per):
            part = scr[pl.ds(base + tok + g, seqs, stride=col_tok), :]
            out = part if out is None else jnp.where(gran == g, part, out)
        return out * mask

    left_tiles = row_tok // per
    right_tiles = col_tok // per
    per_col = col_tok // row_tok
    other = (left_tiles + right_tiles) * 128
    own_base = pl.multiple_of(col * block, block)
    for t in range(right_tiles):
        own_mask = token_ref[pl.ds(col * right_tiles + t, 1), :]
        lanes = (left_tiles + t) * 128
        v = tile(right_scr, own_base, t * per, own_mask).astype(BF16)
        for r in range(rows):
            send_ref[r, :, other + lanes : other + lanes + 128] = v
        for k in range(cols):
            mask = token_ref[k * right_tiles + t : k * right_tiles + t + 1, :]
            v = tile(right_scr, k * block, t * per, mask).astype(BF16)
            for r in range(k * per_col, (k + 1) * per_col):
                send_ref[r, :, lanes : lanes + 128] = v
        sub = t // left_tiles
        lanes = (t % left_tiles) * 128
        v = (tile(left_scr, own_base, t * per, own_mask) * present).astype(BF16)
        for r in range(sub, rows, per_col):
            send_ref[r, :, lanes : lanes + 128] = v
        for k in range(cols):
            mask = token_ref[k * right_tiles + t : k * right_tiles + t + 1, :]
            v = (tile(left_scr, k * block, t * per, mask) * present).astype(BF16)
            send_ref[k * per_col + sub, :, other + lanes : other + lanes + 128] = v


def pair_mid(got, pair_ref, mean_ref, inv, outer_scr, lhs_scr, pair_scr, row_tok, col_tok, width):
    per = 128 // width
    left = got[:, : row_tok * width]
    right = got[:, row_tok * width :]
    span = row_tok * width
    tiles_j = col_tok // per
    outer = mm(left, right, ((0,), (0,))) * inv
    for jh in range(tiles_j):
        outer_scr[jh * span : (jh + 1) * span, :] = outer[:, jh * 128 : (jh + 1) * 128]
    gran = lane_iota((row_tok, 128)) // width
    for hi in range(width // per):
        for jh in range(tiles_j):
            a = [outer_scr[pl.ds(jh * span + hi * per + lo, row_tok, stride=width), :] for lo in range(per)]
            step = 1
            while step < per:
                odd = (gran // step) % 2 == 1
                b = list(a)
                for lo in range(per):
                    if (lo // step) % 2 == 0:
                        b[lo] = jnp.where(odd, pltpu.roll(a[lo + step], step * width, 1), a[lo])
                        b[lo + step] = jnp.where(odd, a[lo + step], pltpu.roll(a[lo], 128 - step * width, 1))
                a = b
                step *= 2
            for lo in range(per):
                at = (jh * per + lo) * row_tok
                lhs_scr[at : at + row_tok, hi * 128 : (hi + 1) * 128] = a[lo].astype(BF16)
    delta = mm(lhs_scr[...], mean_ref[...])
    pair_scr[...] = pair_ref[...].astype(F32).reshape(pair_scr.shape)
    state = jnp.concatenate(
        [pair_scr[pl.ds(j, row_tok, stride=col_tok), :] for j in range(col_tok)], axis=0
    )
    return (state + delta).astype(BF16)


def pair_scratch(row_tok, col_tok, width, pair_width):
    return [
        pltpu.VMEM((row_tok * width * col_tok * width // 128, 128), F32),
        pltpu.VMEM((row_tok * col_tok, width * width), BF16),
        pltpu.VMEM((row_tok * col_tok, pair_width), F32),
    ]


def score_kernel(
    got_ref, pair_ref, mean_ref, score_ref, inv_ref, chunk_ref, *scratch, row_tok, col_tok, width, heads
):
    rows, seqs, lanes = got_ref.shape
    got = got_ref[:, :, : lanes // 2].reshape(rows * seqs, lanes // 2)
    mid = pair_mid(got, pair_ref, mean_ref, inv_ref[:1, :1], *scratch, row_tok, col_tok, width)
    pn = normed(mid.astype(F32))
    scores = mm(score_ref[...], pn, ((1,), (1,)), lax.Precision.HIGHEST)
    sub = lax.broadcasted_iota(jnp.int32, (heads, 128), 0)
    lane_gran = lane_iota((heads, 128)) // row_tok
    turn = jnp.bitwise_and(lane_gran - sub, heads - 1)
    tiles = []
    for t in range(col_tok // heads):
        v = scores[:, t * 128 : (t + 1) * 128]
        out = v
        for k in range(1, heads):
            moved = pltpu.roll(pltpu.roll(v, heads - k, 0), row_tok * k, 1)
            out = jnp.where(turn == k, moved, out)
        tiles.append(out)
    by_token = jnp.concatenate(tiles, axis=0)
    top = jnp.max(by_token, axis=0, keepdims=True).astype(BF16)
    shifted = jnp.exp(by_token - top.astype(F32)).astype(BF16)
    tops = jnp.broadcast_to(top, (8, 128))
    for d in range(chunk_ref.shape[0]):
        chunk_ref[d, :col_tok, :] = shifted
        chunk_ref[d, col_tok:, :] = tops


def transition_kernel(
    got_ref, pair_ref, mean_ref, inv_ref, win_ref, wout_ref, xn_ref, wv_ref,
    out_ref, values_ref, *scratch, row_tok, col_tok, width,
):
    cols, seqs, _, feat = xn_ref.shape
    mixed = wv_ref.shape[1]
    for k in range(cols):
        v = mm(xn_ref[k].reshape(seqs * col_tok, feat), wv_ref[...]).reshape(seqs, col_tok, mixed)
        values_ref[:, k * col_tok : (k + 1) * col_tok, :] = v.astype(BF16)
    rows, _, lanes = got_ref.shape
    got = got_ref[:, :, lanes // 2 :].reshape(rows * seqs, lanes // 2)
    mid = pair_mid(got, pair_ref, mean_ref, inv_ref[:1, :1], *scratch, row_tok, col_tok, width).astype(F32)
    pn = normed(mid).astype(BF16)
    out_scr = scratch[2]
    ff = wout_ref.shape[0]
    step = 8 * row_tok
    for b in range(col_tok // 8):
        pre = mm(pn[b * step : (b + 1) * step, :], win_ref[...])
        act = pre[:, :ff]
        hidden = (act / (1.0 + jnp.exp(-act)) * pre[:, ff:]).astype(BF16)
        new = mid[b * step : (b + 1) * step, :] + mm(hidden, wout_ref[...])
        for t in range(8):
            out_scr[pl.ds(b * 8 + t, row_tok, stride=col_tok), :] = new[t * row_tok : (t + 1) * row_tok, :]
    out_ref[...] = out_scr[...].astype(BF16).reshape(out_ref.shape)


def blend_kernel(
    got_ref, values_ref, gate_ref, x_ref, wr_ref, live_ref, out_ref, *, cols, per_col, row_tok, col_tok, heads
):
    lanes = []
    for q in range(per_col):
        tops = [got_ref[k * per_col + q, col_tok:, :].astype(F32)[:1] for k in range(cols)]
        top = functools.reduce(jnp.maximum, tops)
        parts = [
            got_ref[k * per_col + q, :col_tok, :].astype(F32) * jnp.exp(tops[k] - top) for k in range(cols)
        ]
        whole = functools.reduce(lambda a, b: a + b, [jnp.sum(p, axis=0, keepdims=True) for p in parts])
        lanes.append(jnp.concatenate(parts, axis=0) / whole)
    weights = jnp.concatenate([jnp.transpose(v) for v in lanes], axis=0)
    weights = (weights * live_ref[...].astype(F32)).astype(BF16)
    mixed = values_ref.shape[2]
    head_of = lane_iota((row_tok, mixed)) // (mixed // heads)
    seqs = values_ref.shape[0]
    blocks = []
    for s in range(seqs):
        full = mm(weights, values_ref[s])
        for q in range(per_col):
            acc = None
            for h in range(heads):
                at = (q * heads + h) * row_tok
                part = full[at : at + row_tok, :]
                acc = part if acc is None else jnp.where(head_of == h, part, acc)
            blocks.append(acc)
    average = jnp.concatenate(blocks, axis=0)
    gated = (gate_ref[...] * average).astype(BF16)
    delta = mm(gated, wr_ref[...], ((1,), (1,))).reshape(x_ref.shape)
    out_ref[...] = (x_ref[...].astype(F32) + delta).astype(BF16)


def call(kernel, outs, ins, name, scratch=(), smem=0, flops=0, **keys):
    return pl.pallas_call(
        functools.partial(kernel, **keys),
        out_shape=tuple(jax.ShapeDtypeStruct(shape, dtype) for shape, dtype in outs),
        in_specs=[pl.BlockSpec(memory_space=pltpu.VMEM)] * (len(ins) - smem)
        + [pl.BlockSpec(memory_space=pltpu.SMEM)] * smem,
        out_specs=tuple(pl.BlockSpec(memory_space=pltpu.VMEM) for _ in outs),
        scratch_shapes=list(scratch),
        compiler_params=pltpu.CompilerParams(vmem_limit_bytes=VMEM_LIMIT),
        cost_estimate=pl.CostEstimate(flops=flops, bytes_accessed=0, transcendentals=0) if flops else None,
        name=name,
    )(*ins)


def body(x, pair, present, live, wp, mean, score, wv, wg, wr, win, wout):
    cols = lax.axis_size("col")
    rows = lax.axis_size("row")
    seqs, col_tok, feat = x.shape
    row_tok, _, pair_width = pair.shape
    width = wp.shape[1] // 2
    heads = score.shape[1]
    mixed = wv.shape[1]
    tokens = cols * col_tok
    per_col = col_tok // row_tok
    assert col_tok % row_tok == 0 and rows == per_col * cols
    assert heads * row_tok == 128 and 128 % width == 0
    mine = seqs * col_tok
    lanes = 2 * (row_tok + col_tok) * width

    swap = [
        (r * cols + c, (c * per_col + r % per_col) * cols + r // per_col)
        for r in range(rows)
        for c in range(cols)
    ]
    xs = [lax.ppermute(x, "col", [(i, (i + k) % cols) for i in range(cols)]) for k in range(1, cols)]
    other_pair = lax.ppermute(pair, ("row", "col"), swap)

    own, left, right, gate, wl2, wr2, token, seq, inv = call(
        own_kernel,
        [
            (x.shape, BF16), ((mine, 128), F32), ((mine, 128), F32), ((mine, mixed), F32),
            ((feat, 128), BF16), ((feat, 128), BF16), ((tokens * width // 128, 128), F32),
            ((seqs, 128), F32), ((8, 128), F32),
        ],
        [x, wp, wg, present.reshape(1, -1), present, live],
        "own", smem=2, flops=30_000_000, width=width,
    )
    send, xn = call(
        pack_kernel,
        [((rows, seqs, lanes), BF16), ((cols, seqs, col_tok, feat), BF16)],
        xs + [own, left, right, wl2, wr2, token, seq],
        "pack", scratch=[pltpu.VMEM((cols * mine, 128), F32)] * 2,
        cols=cols, rows=rows, col_tok=col_tok, row_tok=row_tok, width=width,
    )
    got = lax.all_to_all(send, "row", 0, 0)

    scratch = pair_scratch(row_tok, col_tok, width, pair_width)
    (chunk,) = call(
        score_kernel,
        [((rows, col_tok + 8, 128), BF16)],
        [got, other_pair, mean, score.T, inv],
        "score", scratch=scratch, row_tok=row_tok, col_tok=col_tok, width=width, heads=heads,
    )
    scores = lax.all_to_all(chunk, "row", 0, 0)

    pair_output, values = call(
        transition_kernel,
        [(pair.shape, BF16), ((seqs, tokens, mixed), BF16)],
        [got, pair, mean, inv, win, wout, xn, wv],
        "transition", scratch=scratch, flops=1_000_000_000, row_tok=row_tok, col_tok=col_tok, width=width,
    )
    (alignment,) = call(
        blend_kernel,
        [(x.shape, BF16)],
        [scores, values, gate, x, wr.T, live.reshape(1, -1)],
        "blend", cols=cols, per_col=per_col, row_tok=row_tok, col_tok=col_tok, heads=heads,
    )
    return alignment, pair_output


def solution(mesh):
    spread = P("row", "col", None)
    return jax.shard_map(
        body,
        mesh=mesh,
        in_specs=(spread, spread) + (P(),) * 10,
        out_specs=(spread, spread),
        check_vma=False,
    )
```

```python
import functools

import jax
import jax.numpy as jnp
from jax import lax
from jax.experimental import pallas as pl
from jax.experimental.pallas import tpu as pltpu
from jax.sharding import PartitionSpec as P

EPS = 1e-05
F32 = jnp.float32
BF16 = jnp.bfloat16
VMEM_LIMIT = 40 * 1024 * 1024


def normed(v):
    center = v - jnp.mean(v, axis=-1, keepdims=True)
    spread = jnp.mean(center * center, axis=-1, keepdims=True)
    return center * lax.rsqrt(spread + EPS)


def lane_iota(shape):
    return lax.broadcasted_iota(jnp.int32, shape, len(shape) - 1)


def mm(a, b, dims=((1,), (0,)), precision=None):
    return lax.dot_general(a, b, (dims, ((), ())), precision=precision, preferred_element_type=F32)


def meet(a, b, cols):
    return a ^ b ^ (cols - 1)


def one_hot_swap(major, minor, transpose=False):
    size = major * minor
    row = lax.broadcasted_iota(jnp.int32, (size, size), 0)
    col = lax.broadcasted_iota(jnp.int32, (size, size), 1)
    if transpose:
        major, minor = minor, major
    return jnp.where((row % minor) * major + row // minor == col, 1.0, 0.0).astype(BF16)


def own_kernel(
    x_ref, wp_ref, present_ref, live_ref,
    xn_ref, proj_ref, w_ref, turn_ref, token_ref, seq_ref, inv_ref, *, width,
):
    row = lax.axis_index("row")
    seqs, col_tok, feat = x_ref.shape
    per = 128 // width
    wp = wp_ref[...]
    w = jnp.concatenate([wp[:, :width]] * per + [wp[:, width:]] * per, axis=1)
    w_ref[...] = w
    turn = one_hot_swap(col_tok, seqs)
    turn_ref[...] = turn
    xn = normed(x_ref[...].astype(F32).reshape(seqs * col_tok, feat)).astype(BF16)
    xn_ref[...] = xn.reshape(xn_ref.shape)
    proj_ref[...] = mm(mm(turn, xn).astype(BF16), w)
    flags = present_ref[...].astype(F32)
    shape = (seqs, flags.shape[1])
    mine = lane_iota(shape) == row * seqs + lax.broadcasted_iota(jnp.int32, shape, 0)
    own_flags = jnp.sum(jnp.where(mine, flags, 0.0), axis=1, keepdims=True)
    seq_ref[...] = jnp.broadcast_to(own_flags, seq_ref.shape)
    live = live_ref[...].astype(F32)
    tokens = live.shape[1]
    shape = (token_ref.shape[0], tokens)
    here = lane_iota(shape) // per == lax.broadcasted_iota(jnp.int32, shape, 0)
    shape = (tokens, 128)
    spread = lax.broadcasted_iota(jnp.int32, shape, 0) % per == lane_iota(shape) // width
    token_ref[...] = mm(
        jnp.where(here, live, 0.0).astype(BF16), jnp.where(spread, 1.0, 0.0).astype(BF16)
    )
    count = jnp.sum(flags, axis=1, keepdims=True)
    inv_ref[...] = jnp.broadcast_to(1.0 / jnp.maximum(count, 1.0), inv_ref.shape)


def pack_kernel(*refs, cols, rows, col_tok, row_tok, width):
    xs = refs[: cols - 1]
    own_ref, proj_ref, w_ref, turn_ref, token_ref, seq_ref, send_ref, xn_ref = refs[cols - 1 :]
    col = lax.axis_index("col")
    seqs = own_ref.shape[0]
    block = seqs * col_tok
    per = 128 // width
    per_col = col_tok // row_tok
    left_tiles = row_tok // per
    right_tiles = col_tok // per
    other = (left_tiles + right_tiles) * 128
    gran = lane_iota((seqs, 128)) // width
    present = seq_ref[...]

    def tile(y, t):
        out = None
        for g in range(per):
            part = y[(t * per + g) * seqs : (t * per + g + 1) * seqs, :]
            out = part if out is None else jnp.where(gran == g, part, out)
        return out

    for k in range(cols):
        at = lax.rem(col - k + cols, cols)
        if k == 0:
            xn_ref[at] = own_ref[...]
            y = proj_ref[...]
        else:
            v = xs[k - 1][...]
            xn = normed(v.astype(F32).reshape(block, v.shape[2])).astype(BF16)
            xn_ref[at] = xn.reshape(xn_ref.shape[1:])
            y = mm(mm(turn_ref[...], xn).astype(BF16), w_ref[...])
        left = y[:, :128]
        right = y[:, 128:]
        for t in range(right_tiles):
            mask = token_ref[pl.ds(at * right_tiles + t, 1), :]
            lanes = (left_tiles + t) * 128
            v = (tile(right, t) * mask).astype(BF16)
            for e in range(per_col):
                send_ref[meet(at, col, cols) * per_col + e, :, lanes : lanes + 128] = v
            if k == 0:
                for r in range(rows):
                    send_ref[r, :, other + lanes : other + lanes + 128] = v
            sub = t // left_tiles
            lanes = (t % left_tiles) * 128
            v = (tile(left, t) * (mask * present)).astype(BF16)
            send_ref[at * per_col + sub, :, other + lanes : other + lanes + 128] = v
            if k == 0:
                for r in range(sub, rows, per_col):
                    send_ref[r, :, lanes : lanes + 128] = v


def values_kernel(xn_ref, own_ref, wv_ref, wg_ref, values_ref, gate_ref):
    cols, seqs, col_tok, feat = xn_ref.shape
    mixed = wv_ref.shape[1]
    for k in range(cols):
        v = mm(xn_ref[k].reshape(seqs * col_tok, feat), wv_ref[...]).reshape(seqs, col_tok, mixed)
        values_ref[:, k * col_tok : (k + 1) * col_tok, :] = v.astype(BF16)
    gate = mm(own_ref[...].reshape(seqs * col_tok, feat), wg_ref[...])
    gate_ref[...] = 1.0 / (1.0 + jnp.exp(-gate))


def order_kernel(pair_ref, other_ref, swap_ref, own_out, other_out):
    row_tok, col_tok, width = pair_ref.shape
    swap_ref[...] = one_hot_swap(row_tok, col_tok)
    back = one_hot_swap(row_tok, col_tok, transpose=True)
    for source, target in ((pair_ref, own_out), (other_ref, other_out)):
        target[...] = mm(back, source[...].reshape(row_tok * col_tok, width)).astype(BF16)


def pair_mid(got, state, mean_ref, swap, inv, row_tok, col_tok, width):
    per = 128 // width
    left = mm(got[:, : row_tok * width], swap).astype(BF16)
    right = got[:, row_tok * width :]
    gran = lane_iota((row_tok, 128)) // width
    group = per * row_tok
    delta = None
    for pair in range(0, width // per, 2):
        outer = mm(left[:, pair * group : (pair + 2) * group], right, ((0,), (0,)))
        outer = (outer * inv).astype(BF16)
        halves = []
        for half in range(2):
            tiles = []
            for jh in range(col_tok // per):
                a = []
                for lo in range(per):
                    at = (half * per + lo) * row_tok
                    a.append(outer[at : at + row_tok, jh * 128 : (jh + 1) * 128])
                step = 1
                while step < per:
                    odd = (gran // step) % 2 == 1
                    b = list(a)
                    for lo in range(per):
                        if (lo // step) % 2 == 0:
                            b[lo] = jnp.where(odd, pltpu.roll(a[lo + step], step * width, 1), a[lo])
                            b[lo + step] = jnp.where(odd, a[lo + step], pltpu.roll(a[lo], 128 - step * width, 1))
                    a = b
                    step *= 2
                tiles += a
            halves.append(jnp.concatenate(tiles, axis=0))
        part = mm(jnp.concatenate(halves, axis=1), mean_ref[pair * 128 : (pair + 2) * 128, :])
        delta = part if delta is None else delta + part
    return (state.astype(F32) + delta).astype(BF16)


def score_kernel(
    got_ref, state_ref, mean_ref, swap_ref, score_ref, inv_ref, chunk_ref, *, row_tok, col_tok, width, heads
):
    rows, seqs, lanes = got_ref.shape
    got = got_ref[:, :, : lanes // 2].reshape(rows * seqs, lanes // 2)
    mid = pair_mid(got, state_ref[...], mean_ref, swap_ref[...], inv_ref[:1, :1], row_tok, col_tok, width)
    pn = normed(mid.astype(F32))
    scores = mm(score_ref[...], pn, ((1,), (1,)), lax.Precision.HIGHEST)
    sub = lax.broadcasted_iota(jnp.int32, (heads, 128), 0)
    lane_gran = lane_iota((heads, 128)) // row_tok
    turn = jnp.bitwise_and(lane_gran - sub, heads - 1)
    tiles = []
    for t in range(col_tok // heads):
        v = scores[:, t * 128 : (t + 1) * 128]
        out = v
        for k in range(1, heads):
            moved = pltpu.roll(pltpu.roll(v, heads - k, 0), row_tok * k, 1)
            out = jnp.where(turn == k, moved, out)
        tiles.append(out)
    by_token = jnp.concatenate(tiles, axis=0)
    top = jnp.max(by_token, axis=0, keepdims=True).astype(BF16)
    shifted = jnp.exp(by_token - top.astype(F32)).astype(BF16)
    tops = jnp.broadcast_to(top, (8, 128))
    for d in range(chunk_ref.shape[0]):
        chunk_ref[d, :col_tok, :] = shifted
        chunk_ref[d, col_tok:, :] = tops


def transition_kernel(
    got_ref, state_ref, mean_ref, swap_ref, inv_ref, win_ref, wout_ref, out_ref, *, row_tok, col_tok, width
):
    rows, seqs, lanes = got_ref.shape
    got = got_ref[:, :, lanes // 2 :].reshape(rows * seqs, lanes // 2)
    swap = swap_ref[...]
    mid = pair_mid(got, state_ref[...], mean_ref, swap, inv_ref[:1, :1], row_tok, col_tok, width).astype(F32)
    pn = normed(mid).astype(BF16)
    ff = wout_ref.shape[0]
    step = 8 * row_tok
    news = []
    for b in range(col_tok // 8):
        pre = mm(pn[b * step : (b + 1) * step, :], win_ref[...])
        act = pre[:, :ff]
        hidden = (act / (1.0 + jnp.exp(-act)) * pre[:, ff:]).astype(BF16)
        news.append((mid[b * step : (b + 1) * step, :] + mm(hidden, wout_ref[...])).astype(BF16))
    out_ref[...] = mm(swap, jnp.concatenate(news, axis=0)).astype(BF16).reshape(out_ref.shape)


def blend_kernel(
    got_ref, values_ref, gate_ref, x_ref, wr_ref, live_ref, pair_ref, out_ref, pair_out, pair_sem,
    *, cols, per_col, row_tok, col_tok, heads,
):
    leave = pltpu.make_async_copy(pair_ref, pair_out, pair_sem)
    leave.start()
    own = lax.axis_index("col")
    lanes = []
    for q in range(per_col):
        froms = [meet(k, own, cols) * per_col + q for k in range(cols)]
        tops = [got_ref[f, col_tok:, :].astype(F32)[:1] for f in froms]
        top = functools.reduce(jnp.maximum, tops)
        parts = [got_ref[f, :col_tok, :].astype(F32) * jnp.exp(t - top) for f, t in zip(froms, tops)]
        whole = functools.reduce(lambda a, b: a + b, [jnp.sum(p, axis=0, keepdims=True) for p in parts])
        lanes.append(jnp.concatenate(parts, axis=0) / whole)
    weights = jnp.concatenate([jnp.transpose(v) for v in lanes], axis=0)
    weights = (weights * live_ref[...].astype(F32)).astype(BF16)
    mixed = values_ref.shape[2]
    head_of = lane_iota((row_tok, mixed)) // (mixed // heads)
    seqs = values_ref.shape[0]
    blocks = []
    for s in range(seqs):
        full = mm(weights, values_ref[s])
        for q in range(per_col):
            acc = None
            for h in range(heads):
                at = (q * heads + h) * row_tok
                part = full[at : at + row_tok, :]
                acc = part if acc is None else jnp.where(head_of == h, part, acc)
            blocks.append(acc)
    average = jnp.concatenate(blocks, axis=0)
    gated = (gate_ref[...] * average).astype(BF16)
    delta = mm(gated, wr_ref[...], ((1,), (1,))).reshape(x_ref.shape)
    out_ref[...] = (x_ref[...].astype(F32) + delta).astype(BF16)
    leave.wait()


def call(kernel, outs, ins, scratch=(), hbm_outs=0, flops=0, **keys):
    return pl.pallas_call(
        functools.partial(kernel, **keys),
        out_shape=tuple(jax.ShapeDtypeStruct(shape, dtype) for shape, dtype in outs),
        in_specs=[pl.BlockSpec(memory_space=pltpu.VMEM)] * len(ins),
        out_specs=(pl.BlockSpec(memory_space=pltpu.VMEM),) * (len(outs) - hbm_outs)
        + (pl.BlockSpec(memory_space=pl.ANY),) * hbm_outs,
        scratch_shapes=list(scratch),
        compiler_params=pltpu.CompilerParams(vmem_limit_bytes=VMEM_LIMIT),
        cost_estimate=pl.CostEstimate(flops=flops, bytes_accessed=0, transcendentals=0) if flops else None,
    )(*ins)


def body(x, pair, present, live, wp, mean, score, wv, wg, wr, win, wout):
    cols = lax.axis_size("col")
    rows = lax.axis_size("row")
    seqs, col_tok, feat = x.shape
    row_tok, _, pair_width = pair.shape
    width = wp.shape[1] // 2
    heads = score.shape[1]
    mixed = wv.shape[1]
    tokens = cols * col_tok
    per_col = col_tok // row_tok
    assert col_tok % row_tok == 0 and rows == per_col * cols and cols & (cols - 1) == 0
    assert heads * row_tok == 128 and 128 % width == 0 and width == col_tok
    mine = seqs * col_tok
    lanes = 2 * (row_tok + col_tok) * width

    swap = [
        (r * cols + c, (meet(r // per_col, c, cols) * per_col + r % per_col) * cols + r // per_col)
        for r in range(rows)
        for c in range(cols)
    ]
    xs = [lax.ppermute(x, "col", [(i, (i + k) % cols) for i in range(cols)]) for k in range(1, cols)]
    other_pair = lax.ppermute(pair, ("row", "col"), swap)

    own, proj, w, turn, token, seq, inv = call(
        own_kernel,
        [
            (x.shape, BF16), ((mine, 256), F32), ((feat, 256), BF16), ((mine, mine), BF16),
            ((tokens * width // 128, 128), F32), ((seqs, 128), F32), ((8, 128), F32),
        ],
        [x, wp, present.reshape(1, -1), live.reshape(1, -1)],
        flops=30_000_000, width=width,
    )
    send, xn = call(
        pack_kernel,
        [((rows, seqs, lanes), BF16), ((cols, seqs, col_tok, feat), BF16)],
        xs + [own, proj, w, turn, token, seq],
        cols=cols, rows=rows, col_tok=col_tok, row_tok=row_tok, width=width,
    )
    got = lax.all_to_all(send, "row", 0, 0)
    values, gate = call(
        values_kernel, [((seqs, tokens, mixed), BF16), ((mine, mixed), F32)], [xn, own, wv, wg], flops=100_000_000
    )
    pairs = row_tok * col_tok
    swap_matrix, state, other_state = call(
        order_kernel,
        [((pairs, pairs), BF16), ((pairs, pair_width), BF16), ((pairs, pair_width), BF16)],
        [pair, other_pair],
        flops=100_000_000,
    )
    sizes = dict(row_tok=row_tok, col_tok=col_tok, width=width)
    (chunk,) = call(
        score_kernel,
        [((rows, col_tok + 8, 128), BF16)],
        [got, other_state, mean, swap_matrix, score.T, inv],
        heads=heads, **sizes,
    )
    scores = lax.all_to_all(chunk, "row", 0, 0)
    (pair_new,) = call(
        transition_kernel,
        [(pair.shape, BF16)],
        [got, state, mean, swap_matrix, inv, win, wout],
        flops=1_000_000_000, **sizes,
    )
    alignment, pair_output = call(
        blend_kernel,
        [(x.shape, BF16), (pair.shape, BF16)],
        [scores, values, gate, x, wr.T, live.reshape(1, -1), pair_new],
        scratch=[pltpu.SemaphoreType.DMA], hbm_outs=1, cols=cols, per_col=per_col, row_tok=row_tok, col_tok=col_tok, heads=heads,
    )
    return alignment, pair_output


def solution(mesh):
    spread = P("row", "col", None)
    return jax.shard_map(
        body,
        mesh=mesh,
        in_specs=(spread, spread) + (P(),) * 10,
        out_specs=(spread, spread),
        check_vma=False,
    )
```

```python
import functools

import jax
import jax.numpy as jnp
from jax import lax
from jax.experimental import pallas as pl
from jax.experimental.pallas import tpu as pltpu
from jax.sharding import PartitionSpec as P

EPS = 1e-05
F32 = jnp.float32
BF16 = jnp.bfloat16
VMEM_LIMIT = 40 * 1024 * 1024


def normed(v):
    center = v - jnp.mean(v, axis=-1, keepdims=True)
    spread = jnp.mean(center * center, axis=-1, keepdims=True)
    return center * lax.rsqrt(spread + EPS)


def lane_iota(shape):
    return lax.broadcasted_iota(jnp.int32, shape, len(shape) - 1)


def mm(a, b, dims=((1,), (0,)), precision=None):
    return lax.dot_general(a, b, (dims, ((), ())), precision=precision, preferred_element_type=F32)


def meet(a, b, cols):
    return a ^ b ^ (cols - 1)


def one_hot_swap(major, minor, transpose=False):
    size = major * minor
    row = lax.broadcasted_iota(jnp.int32, (size, size), 0)
    col = lax.broadcasted_iota(jnp.int32, (size, size), 1)
    if transpose:
        major, minor = minor, major
    return jnp.where((row % minor) * major + row // minor == col, 1.0, 0.0).astype(BF16)


def turn_kernel(turn_ref, *, seqs, col_tok):
    turn_ref[...] = one_hot_swap(col_tok, seqs)


def own_kernel(
    x_ref, wp_ref, present_ref, live_ref, turn_ref,
    xn_ref, proj_ref, w_ref, token_ref, seq_ref, inv_ref, *, width,
):
    row = lax.axis_index("row")
    seqs, col_tok, feat = x_ref.shape
    per = 128 // width
    wp = wp_ref[...]
    w = jnp.concatenate([wp[:, :width]] * per + [wp[:, width:]] * per, axis=1)
    w_ref[...] = w
    turn = turn_ref[...]
    xn = normed(x_ref[...].astype(F32).reshape(seqs * col_tok, feat)).astype(BF16)
    xn_ref[...] = xn.reshape(xn_ref.shape)
    proj_ref[...] = mm(mm(turn, xn).astype(BF16), w)
    flags = present_ref[...].astype(F32)
    shape = (seqs, flags.shape[1])
    mine = lane_iota(shape) == row * seqs + lax.broadcasted_iota(jnp.int32, shape, 0)
    own_flags = jnp.sum(jnp.where(mine, flags, 0.0), axis=1, keepdims=True)
    seq_ref[...] = jnp.broadcast_to(own_flags, seq_ref.shape)
    live = live_ref[...].astype(F32)
    tokens = live.shape[1]
    shape = (token_ref.shape[0], tokens)
    here = lane_iota(shape) // per == lax.broadcasted_iota(jnp.int32, shape, 0)
    shape = (tokens, 128)
    spread = lax.broadcasted_iota(jnp.int32, shape, 0) % per == lane_iota(shape) // width
    token_ref[...] = mm(
        jnp.where(here, live, 0.0).astype(BF16), jnp.where(spread, 1.0, 0.0).astype(BF16)
    )
    count = jnp.sum(flags, axis=1, keepdims=True)
    inv_ref[...] = jnp.broadcast_to(1.0 / jnp.maximum(count, 1.0), inv_ref.shape)


def pack_kernel(*refs, cols, rows, col_tok, row_tok, width):
    xs = refs[: cols - 1]
    own_ref, proj_ref, w_ref, turn_ref, token_ref, seq_ref, send_ref, xn_ref = refs[cols - 1 :]
    col = lax.axis_index("col")
    seqs = own_ref.shape[0]
    block = seqs * col_tok
    per = 128 // width
    per_col = col_tok // row_tok
    left_tiles = row_tok // per
    right_tiles = col_tok // per
    other = (left_tiles + right_tiles) * 128
    gran = lane_iota((seqs, 128)) // width
    present = seq_ref[...]

    def tile(y, t):
        out = None
        for g in range(per):
            part = y[(t * per + g) * seqs : (t * per + g + 1) * seqs, :]
            out = part if out is None else jnp.where(gran == g, part, out)
        return out

    for k in range(cols):
        at = lax.rem(col - k + cols, cols)
        if k == 0:
            xn_ref[at] = own_ref[...]
            y = proj_ref[...]
        else:
            v = xs[k - 1][...]
            xn = normed(v.astype(F32).reshape(block, v.shape[2])).astype(BF16)
            xn_ref[at] = xn.reshape(xn_ref.shape[1:])
            y = mm(mm(turn_ref[...], xn).astype(BF16), w_ref[...])
        left = y[:, :128]
        right = y[:, 128:]
        for t in range(right_tiles):
            mask = token_ref[pl.ds(at * right_tiles + t, 1), :]
            lanes = (left_tiles + t) * 128
            v = (tile(right, t) * mask).astype(BF16)
            for e in range(per_col):
                send_ref[meet(at, col, cols) * per_col + e, :, lanes : lanes + 128] = v
            if k == 0:
                for r in range(rows):
                    send_ref[r, :, other + lanes : other + lanes + 128] = v
            sub = t // left_tiles
            lanes = (t % left_tiles) * 128
            v = (tile(left, t) * (mask * present)).astype(BF16)
            send_ref[at * per_col + sub, :, other + lanes : other + lanes + 128] = v
            if k == 0:
                for r in range(sub, rows, per_col):
                    send_ref[r, :, lanes : lanes + 128] = v


def values_kernel(xn_ref, own_ref, wv_ref, wg_ref, values_ref, gate_ref):
    cols, seqs, col_tok, feat = xn_ref.shape
    mixed = wv_ref.shape[1]
    for k in range(cols):
        v = mm(xn_ref[k].reshape(seqs * col_tok, feat), wv_ref[...]).reshape(seqs, col_tok, mixed)
        values_ref[:, k * col_tok : (k + 1) * col_tok, :] = v.astype(BF16)
    gate = mm(own_ref[...].reshape(seqs * col_tok, feat), wg_ref[...])
    gate_ref[...] = 1.0 / (1.0 + jnp.exp(-gate))


def order_kernel(pair_ref, other_ref, swap_ref, own_out, other_out):
    row_tok, col_tok, width = pair_ref.shape
    swap_ref[...] = one_hot_swap(row_tok, col_tok)
    back = one_hot_swap(row_tok, col_tok, transpose=True)
    for source, target in ((pair_ref, own_out), (other_ref, other_out)):
        target[...] = mm(back, source[...].reshape(row_tok * col_tok, width)).astype(BF16)


def pair_mid(got, state, mean_ref, swap, inv, row_tok, col_tok, width):
    per = 128 // width
    left = mm(got[:, : row_tok * width], swap).astype(BF16)
    right = got[:, row_tok * width :]
    gran = lane_iota((row_tok, 128)) // width
    group = per * row_tok
    halves = []
    for pair in range(0, width // per, 2):
        outer = mm(left[:, pair * group : (pair + 2) * group], right, ((0,), (0,)))
        outer = (outer * inv).astype(BF16)
        for half in range(2):
            tiles = []
            for jh in range(col_tok // per):
                a = []
                for lo in range(per):
                    at = (half * per + lo) * row_tok
                    a.append(outer[at : at + row_tok, jh * 128 : (jh + 1) * 128])
                step = 1
                while step < per:
                    odd = (gran // step) % 2 == 1
                    b = list(a)
                    for lo in range(per):
                        if (lo // step) % 2 == 0:
                            b[lo] = jnp.where(odd, pltpu.roll(a[lo + step], step * width, 1), a[lo])
                            b[lo + step] = jnp.where(odd, a[lo + step], pltpu.roll(a[lo], 128 - step * width, 1))
                    a = b
                    step *= 2
                tiles += a
            halves.append(jnp.concatenate(tiles, axis=0))
    delta = mm(jnp.concatenate(halves, axis=1), mean_ref[...])
    return (state.astype(F32) + delta).astype(BF16)


def score_kernel(
    got_ref, state_ref, mean_ref, swap_ref, score_ref, inv_ref, chunk_ref, *, row_tok, col_tok, width, heads
):
    rows, seqs, lanes = got_ref.shape
    got = got_ref[:, :, : lanes // 2].reshape(rows * seqs, lanes // 2)
    mid = pair_mid(got, state_ref[...], mean_ref, swap_ref[...], inv_ref[:1, :1], row_tok, col_tok, width)
    pn = normed(mid.astype(F32))
    scores = mm(score_ref[...], pn, ((1,), (1,)), lax.Precision.HIGHEST)
    sub = lax.broadcasted_iota(jnp.int32, (heads, 128), 0)
    lane_gran = lane_iota((heads, 128)) // row_tok
    turn = jnp.bitwise_and(lane_gran - sub, heads - 1)
    tiles = []
    for t in range(col_tok // heads):
        v = scores[:, t * 128 : (t + 1) * 128]
        out = v
        for k in range(1, heads):
            moved = pltpu.roll(pltpu.roll(v, heads - k, 0), row_tok * k, 1)
            out = jnp.where(turn == k, moved, out)
        tiles.append(out)
    by_token = jnp.concatenate(tiles, axis=0)
    top = jnp.max(by_token, axis=0, keepdims=True).astype(BF16)
    shifted = jnp.exp(by_token - top.astype(F32)).astype(BF16)
    tops = jnp.broadcast_to(top, (8, 128))
    for d in range(chunk_ref.shape[0]):
        chunk_ref[d, :col_tok, :] = shifted
        chunk_ref[d, col_tok:, :] = tops


def transition_kernel(
    got_ref, state_ref, mean_ref, swap_ref, inv_ref, win_ref, wout_ref, out_ref, *, row_tok, col_tok, width
):
    rows, seqs, lanes = got_ref.shape
    got = got_ref[:, :, lanes // 2 :].reshape(rows * seqs, lanes // 2)
    swap = swap_ref[...]
    mid = pair_mid(got, state_ref[...], mean_ref, swap, inv_ref[:1, :1], row_tok, col_tok, width).astype(F32)
    pn = normed(mid).astype(BF16)
    ff = wout_ref.shape[0]
    step = 8 * row_tok
    news = []
    for b in range(col_tok // 8):
        pre = mm(pn[b * step : (b + 1) * step, :], win_ref[...])
        act = pre[:, :ff]
        hidden = (act / (1.0 + jnp.exp(-act)) * pre[:, ff:]).astype(BF16)
        news.append((mid[b * step : (b + 1) * step, :] + mm(hidden, wout_ref[...])).astype(BF16))
    out_ref[...] = mm(swap, jnp.concatenate(news, axis=0)).astype(BF16).reshape(out_ref.shape)


def blend_kernel(
    got_ref, values_ref, gate_ref, x_ref, wr_ref, live_ref, pair_ref, out_ref, pair_out, pair_sem,
    *, cols, per_col, row_tok, col_tok, heads,
):
    leave = pltpu.make_async_copy(pair_ref, pair_out, pair_sem)
    leave.start()
    own = lax.axis_index("col")
    lanes = []
    for q in range(per_col):
        froms = [meet(k, own, cols) * per_col + q for k in range(cols)]
        tops = [got_ref[f, col_tok:, :].astype(F32)[:1] for f in froms]
        top = functools.reduce(jnp.maximum, tops)
        parts = [got_ref[f, :col_tok, :].astype(F32) * jnp.exp(t - top) for f, t in zip(froms, tops)]
        whole = functools.reduce(lambda a, b: a + b, [jnp.sum(p, axis=0, keepdims=True) for p in parts])
        lanes.append(jnp.concatenate(parts, axis=0) / whole)
    weights = jnp.concatenate([jnp.transpose(v) for v in lanes], axis=0)
    weights = (weights * live_ref[...].astype(F32)).astype(BF16)
    mixed = values_ref.shape[2]
    head_of = lane_iota((row_tok, mixed)) // (mixed // heads)
    seqs = values_ref.shape[0]
    blocks = []
    for s in range(seqs):
        full = mm(weights, values_ref[s])
        for q in range(per_col):
            acc = None
            for h in range(heads):
                at = (q * heads + h) * row_tok
                part = full[at : at + row_tok, :]
                acc = part if acc is None else jnp.where(head_of == h, part, acc)
            blocks.append(acc)
    average = jnp.concatenate(blocks, axis=0)
    gated = (gate_ref[...] * average).astype(BF16)
    delta = mm(gated, wr_ref[...], ((1,), (1,))).reshape(x_ref.shape)
    out_ref[...] = (x_ref[...].astype(F32) + delta).astype(BF16)
    leave.wait()


def call(kernel, outs, ins, scratch=(), hbm_outs=0, flops=0, **keys):
    return pl.pallas_call(
        functools.partial(kernel, **keys),
        out_shape=tuple(jax.ShapeDtypeStruct(shape, dtype) for shape, dtype in outs),
        in_specs=[pl.BlockSpec(memory_space=pltpu.VMEM)] * len(ins),
        out_specs=(pl.BlockSpec(memory_space=pltpu.VMEM),) * (len(outs) - hbm_outs)
        + (pl.BlockSpec(memory_space=pl.ANY),) * hbm_outs,
        scratch_shapes=list(scratch),
        compiler_params=pltpu.CompilerParams(vmem_limit_bytes=VMEM_LIMIT),
        cost_estimate=pl.CostEstimate(flops=flops, bytes_accessed=0, transcendentals=0) if flops else None,
    )(*ins)


def body(x, pair, present, live, wp, mean, score, wv, wg, wr, win, wout):
    cols = lax.axis_size("col")
    rows = lax.axis_size("row")
    seqs, col_tok, feat = x.shape
    row_tok, _, pair_width = pair.shape
    width = wp.shape[1] // 2
    heads = score.shape[1]
    mixed = wv.shape[1]
    tokens = cols * col_tok
    per_col = col_tok // row_tok
    assert col_tok % row_tok == 0 and rows == per_col * cols and cols & (cols - 1) == 0
    assert heads * row_tok == 128 and 128 % width == 0 and width == col_tok
    mine = seqs * col_tok
    lanes = 2 * (row_tok + col_tok) * width

    swap = [
        (r * cols + c, (meet(r // per_col, c, cols) * per_col + r % per_col) * cols + r // per_col)
        for r in range(rows)
        for c in range(cols)
    ]
    xs = [lax.ppermute(x, "col", [(i, (i + k) % cols) for i in range(cols)]) for k in range(1, cols)]
    other_pair = lax.ppermute(pair, ("row", "col"), swap)

    (turn,) = call(turn_kernel, [((mine, mine), BF16)], [], flops=20_000_000_000, seqs=seqs, col_tok=col_tok)
    own, proj, w, token, seq, inv = call(
        own_kernel,
        [
            (x.shape, BF16), ((mine, 256), F32), ((feat, 256), BF16),
            ((tokens * width // 128, 128), F32), ((seqs, 128), F32), ((8, 128), F32),
        ],
        [x, wp, present.reshape(1, -1), live.reshape(1, -1), turn],
        flops=30_000_000, width=width,
    )
    send, xn = call(
        pack_kernel,
        [((rows, seqs, lanes), BF16), ((cols, seqs, col_tok, feat), BF16)],
        xs + [own, proj, w, turn, token, seq],
        cols=cols, rows=rows, col_tok=col_tok, row_tok=row_tok, width=width,
    )
    got = lax.all_to_all(send, "row", 0, 0)
    values, gate = call(
        values_kernel, [((seqs, tokens, mixed), BF16), ((mine, mixed), F32)], [xn, own, wv, wg], flops=100_000_000
    )
    pairs = row_tok * col_tok
    swap_matrix, state, other_state = call(
        order_kernel,
        [((pairs, pairs), BF16), ((pairs, pair_width), BF16), ((pairs, pair_width), BF16)],
        [pair, other_pair],
        flops=100_000_000,
    )
    sizes = dict(row_tok=row_tok, col_tok=col_tok, width=width)
    (chunk,) = call(
        score_kernel,
        [((rows, col_tok + 8, 128), BF16)],
        [got, other_state, mean, swap_matrix, score.T, inv],
        heads=heads, **sizes,
    )
    scores = lax.all_to_all(chunk, "row", 0, 0)
    (pair_new,) = call(
        transition_kernel,
        [(pair.shape, BF16)],
        [got, state, mean, swap_matrix, inv, win, wout],
        flops=1_000_000_000, **sizes,
    )
    alignment, pair_output = call(
        blend_kernel,
        [(x.shape, BF16), (pair.shape, BF16)],
        [scores, values, gate, x, wr.T, live.reshape(1, -1), pair_new],
        scratch=[pltpu.SemaphoreType.DMA], hbm_outs=1, cols=cols, per_col=per_col, row_tok=row_tok, col_tok=col_tok, heads=heads,
    )
    return alignment, pair_output


def solution(mesh):
    spread = P("row", "col", None)
    return jax.shard_map(
        body,
        mesh=mesh,
        in_specs=(spread, spread) + (P(),) * 10,
        out_specs=(spread, spread),
        check_vma=False,
    )
```

```python
import functools

import jax
import jax.numpy as jnp
from jax import lax
from jax.experimental import pallas as pl
from jax.experimental.pallas import tpu as pltpu
from jax.sharding import PartitionSpec as P

EPS = 1e-05
F32 = jnp.float32
BF16 = jnp.bfloat16
VMEM_LIMIT = 40 * 1024 * 1024


def normed(v):
    center = v - jnp.mean(v, axis=-1, keepdims=True)
    spread = jnp.mean(center * center, axis=-1, keepdims=True)
    return center * lax.rsqrt(spread + EPS)


def lane_iota(shape):
    return lax.broadcasted_iota(jnp.int32, shape, len(shape) - 1)


def mm(a, b, dims=((1,), (0,)), precision=None):
    return lax.dot_general(a, b, (dims, ((), ())), precision=precision, preferred_element_type=F32)


def meet(a, b, cols):
    return a ^ b ^ (cols - 1)


def one_hot_swap(major, minor, transpose=False):
    size = major * minor
    row = lax.broadcasted_iota(jnp.int32, (size, size), 0)
    col = lax.broadcasted_iota(jnp.int32, (size, size), 1)
    if transpose:
        major, minor = minor, major
    return jnp.where((row % minor) * major + row // minor == col, 1.0, 0.0).astype(BF16)


def turn_kernel(turn_ref, *, seqs, col_tok):
    turn_ref[...] = one_hot_swap(col_tok, seqs)


def own_kernel(
    x_ref, wp_ref, present_ref, live_ref, turn_ref,
    xn_ref, proj_ref, w_ref, token_ref, seq_ref, inv_ref, *, width,
):
    row = lax.axis_index("row")
    seqs, col_tok, feat = x_ref.shape
    per = 128 // width
    wp = wp_ref[...]
    w = jnp.concatenate([wp[:, :width]] * per + [wp[:, width:]] * per, axis=1)
    w_ref[...] = w
    turn = turn_ref[...]
    xn = normed(x_ref[...].astype(F32).reshape(seqs * col_tok, feat)).astype(BF16)
    xn_ref[...] = xn.reshape(xn_ref.shape)
    proj_ref[...] = mm(mm(turn, xn).astype(BF16), w)
    flags = present_ref[...].astype(F32).reshape(1, -1)
    shape = (seqs, flags.shape[1])
    mine = lane_iota(shape) == row * seqs + lax.broadcasted_iota(jnp.int32, shape, 0)
    own_flags = jnp.sum(jnp.where(mine, flags, 0.0), axis=1, keepdims=True)
    seq_ref[...] = jnp.broadcast_to(own_flags, seq_ref.shape)
    live = live_ref[...].astype(F32).reshape(1, -1)
    tokens = live.shape[1]
    shape = (token_ref.shape[0], tokens)
    here = lane_iota(shape) // per == lax.broadcasted_iota(jnp.int32, shape, 0)
    shape = (tokens, 128)
    spread = lax.broadcasted_iota(jnp.int32, shape, 0) % per == lane_iota(shape) // width
    token_ref[...] = mm(
        jnp.where(here, live, 0.0).astype(BF16), jnp.where(spread, 1.0, 0.0).astype(BF16)
    )
    count = jnp.sum(flags, axis=1, keepdims=True)
    inv_ref[...] = jnp.broadcast_to(1.0 / jnp.maximum(count, 1.0), inv_ref.shape)


def pack_kernel(*refs, cols, rows, col_tok, row_tok, width):
    xs = refs[: cols - 1]
    own_ref, proj_ref, w_ref, turn_ref, token_ref, seq_ref, send_ref, xn_ref = refs[cols - 1 :]
    col = lax.axis_index("col")
    seqs = own_ref.shape[0]
    block = seqs * col_tok
    per = 128 // width
    per_col = col_tok // row_tok
    left_tiles = row_tok // per
    right_tiles = col_tok // per
    other = (left_tiles + right_tiles) * 128
    gran = lane_iota((seqs, 128)) // width
    present = seq_ref[...]

    def tile(y, t):
        out = None
        for g in range(per):
            part = y[(t * per + g) * seqs : (t * per + g + 1) * seqs, :]
            out = part if out is None else jnp.where(gran == g, part, out)
        return out

    for k in range(cols):
        at = lax.rem(col - k + cols, cols)
        if k == 0:
            xn_ref[at] = own_ref[...]
            y = proj_ref[...]
        else:
            v = xs[k - 1][...]
            xn = normed(v.astype(F32).reshape(block, v.shape[2])).astype(BF16)
            xn_ref[at] = xn.reshape(xn_ref.shape[1:])
            y = mm(mm(turn_ref[...], xn).astype(BF16), w_ref[...])
        left = y[:, :128]
        right = y[:, 128:]
        for t in range(right_tiles):
            mask = token_ref[pl.ds(at * right_tiles + t, 1), :]
            lanes = (left_tiles + t) * 128
            v = (tile(right, t) * mask).astype(BF16)
            for e in range(per_col):
                send_ref[meet(at, col, cols) * per_col + e, :, lanes : lanes + 128] = v
            if k == 0:
                for r in range(rows):
                    send_ref[r, :, other + lanes : other + lanes + 128] = v
            sub = t // left_tiles
            lanes = (t % left_tiles) * 128
            v = (tile(left, t) * (mask * present)).astype(BF16)
            send_ref[at * per_col + sub, :, other + lanes : other + lanes + 128] = v
            if k == 0:
                for r in range(sub, rows, per_col):
                    send_ref[r, :, lanes : lanes + 128] = v


def values_kernel(xn_ref, own_ref, wv_ref, wg_ref, values_ref, gate_ref):
    cols, seqs, col_tok, feat = xn_ref.shape
    mixed = wv_ref.shape[1]
    for k in range(cols):
        v = mm(xn_ref[k].reshape(seqs * col_tok, feat), wv_ref[...]).reshape(seqs, col_tok, mixed)
        values_ref[:, k * col_tok : (k + 1) * col_tok, :] = v.astype(BF16)
    gate = mm(own_ref[...].reshape(seqs * col_tok, feat), wg_ref[...])
    gate_ref[...] = 1.0 / (1.0 + jnp.exp(-gate))


def order_kernel(pair_ref, other_ref, swap_ref, own_out, other_out):
    row_tok, col_tok, width = pair_ref.shape
    swap_ref[...] = one_hot_swap(row_tok, col_tok)
    back = one_hot_swap(row_tok, col_tok, transpose=True)
    for source, target in ((pair_ref, own_out), (other_ref, other_out)):
        target[...] = mm(back, source[...].reshape(row_tok * col_tok, width)).astype(BF16)


def pair_mid(got, state, mean_ref, swap, inv, row_tok, col_tok, width):
    per = 128 // width
    left = mm(got[:, : row_tok * width], swap).astype(BF16)
    right = got[:, row_tok * width :]
    gran = lane_iota((row_tok, 128)) // width
    group = per * row_tok
    halves = []
    for pair in range(0, width // per, 2):
        outer = mm(left[:, pair * group : (pair + 2) * group], right, ((0,), (0,)))
        outer = (outer * inv).astype(BF16)
        for half in range(2):
            tiles = []
            for jh in range(col_tok // per):
                a = []
                for lo in range(per):
                    at = (half * per + lo) * row_tok
                    a.append(outer[at : at + row_tok, jh * 128 : (jh + 1) * 128])
                step = 1
                while step < per:
                    odd = (gran // step) % 2 == 1
                    b = list(a)
                    for lo in range(per):
                        if (lo // step) % 2 == 0:
                            b[lo] = jnp.where(odd, pltpu.roll(a[lo + step], step * width, 1), a[lo])
                            b[lo + step] = jnp.where(odd, a[lo + step], pltpu.roll(a[lo], 128 - step * width, 1))
                    a = b
                    step *= 2
                tiles += a
            halves.append(jnp.concatenate(tiles, axis=0))
    delta = mm(jnp.concatenate(halves, axis=1), mean_ref[...])
    return (state.astype(F32) + delta).astype(BF16)


def score_kernel(
    got_ref, state_ref, mean_ref, swap_ref, score_ref, inv_ref, chunk_ref, *, row_tok, col_tok, width, heads
):
    rows, seqs, lanes = got_ref.shape
    got = got_ref[:, :, : lanes // 2].reshape(rows * seqs, lanes // 2)
    mid = pair_mid(got, state_ref[...], mean_ref, swap_ref[...], inv_ref[:1, :1], row_tok, col_tok, width)
    pn = normed(mid.astype(F32))
    scores = mm(score_ref[...], pn, ((1,), (1,)), lax.Precision.HIGHEST)
    sub = lax.broadcasted_iota(jnp.int32, (heads, 128), 0)
    lane_gran = lane_iota((heads, 128)) // row_tok
    turn = jnp.bitwise_and(lane_gran - sub, heads - 1)
    tiles = []
    for t in range(col_tok // heads):
        v = scores[:, t * 128 : (t + 1) * 128]
        out = v
        for k in range(1, heads):
            moved = pltpu.roll(pltpu.roll(v, heads - k, 0), row_tok * k, 1)
            out = jnp.where(turn == k, moved, out)
        tiles.append(out)
    by_token = jnp.concatenate(tiles, axis=0)
    top = jnp.max(by_token, axis=0, keepdims=True).astype(BF16)
    shifted = jnp.exp(by_token - top.astype(F32)).astype(BF16)
    tops = jnp.broadcast_to(top, (8, 128))
    for d in range(chunk_ref.shape[0]):
        chunk_ref[d, :col_tok, :] = shifted
        chunk_ref[d, col_tok:, :] = tops


def transition_kernel(
    got_ref, state_ref, mean_ref, swap_ref, inv_ref, win_ref, wout_ref, out_ref, *, row_tok, col_tok, width
):
    rows, seqs, lanes = got_ref.shape
    got = got_ref[:, :, lanes // 2 :].reshape(rows * seqs, lanes // 2)
    swap = swap_ref[...]
    mid = pair_mid(got, state_ref[...], mean_ref, swap, inv_ref[:1, :1], row_tok, col_tok, width).astype(F32)
    pn = normed(mid).astype(BF16)
    ff = wout_ref.shape[0]
    step = 8 * row_tok
    news = []
    for b in range(col_tok // 8):
        pre = mm(pn[b * step : (b + 1) * step, :], win_ref[...])
        act = pre[:, :ff]
        hidden = (act / (1.0 + jnp.exp(-act)) * pre[:, ff:]).astype(BF16)
        news.append((mid[b * step : (b + 1) * step, :] + mm(hidden, wout_ref[...])).astype(BF16))
    out_ref[...] = mm(swap, jnp.concatenate(news, axis=0)).astype(BF16).reshape(out_ref.shape)


def blend_kernel(
    got_ref, values_ref, gate_ref, x_ref, wr_ref, live_ref, pair_ref, out_ref, pair_out, pair_sem,
    *, cols, per_col, row_tok, col_tok, heads,
):
    leave = pltpu.make_async_copy(pair_ref, pair_out, pair_sem)
    leave.start()
    own = lax.axis_index("col")
    lanes = []
    for q in range(per_col):
        froms = [meet(k, own, cols) * per_col + q for k in range(cols)]
        tops = [got_ref[f, col_tok:, :].astype(F32)[:1] for f in froms]
        top = functools.reduce(jnp.maximum, tops)
        parts = [got_ref[f, :col_tok, :].astype(F32) * jnp.exp(t - top) for f, t in zip(froms, tops)]
        whole = functools.reduce(lambda a, b: a + b, [jnp.sum(p, axis=0, keepdims=True) for p in parts])
        lanes.append(jnp.concatenate(parts, axis=0) / whole)
    weights = jnp.concatenate([jnp.transpose(v) for v in lanes], axis=0)
    weights = (weights * live_ref[...].astype(F32)).astype(BF16)
    mixed = values_ref.shape[2]
    head_of = lane_iota((row_tok, mixed)) // (mixed // heads)
    seqs = values_ref.shape[0]
    blocks = []
    for s in range(seqs):
        full = mm(weights, values_ref[s])
        for q in range(per_col):
            acc = None
            for h in range(heads):
                at = (q * heads + h) * row_tok
                part = full[at : at + row_tok, :]
                acc = part if acc is None else jnp.where(head_of == h, part, acc)
            blocks.append(acc)
    average = jnp.concatenate(blocks, axis=0)
    gated = (gate_ref[...] * average).astype(BF16)
    delta = mm(gated, wr_ref[...], ((1,), (1,))).reshape(x_ref.shape)
    out_ref[...] = (x_ref[...].astype(F32) + delta).astype(BF16)
    leave.wait()


def call(kernel, outs, ins, scratch=(), hbm_outs=0, flops=0, **keys):
    return pl.pallas_call(
        functools.partial(kernel, **keys),
        out_shape=tuple(jax.ShapeDtypeStruct(shape, dtype) for shape, dtype in outs),
        in_specs=[pl.BlockSpec(memory_space=pltpu.VMEM)] * len(ins),
        out_specs=(pl.BlockSpec(memory_space=pltpu.VMEM),) * (len(outs) - hbm_outs)
        + (pl.BlockSpec(memory_space=pl.ANY),) * hbm_outs,
        scratch_shapes=list(scratch),
        compiler_params=pltpu.CompilerParams(vmem_limit_bytes=VMEM_LIMIT),
        cost_estimate=pl.CostEstimate(flops=flops, bytes_accessed=0, transcendentals=0) if flops else None,
    )(*ins)


def body(x, pair, present, live, wp, mean, score, wv, wg, wr, win, wout):
    cols = lax.axis_size("col")
    rows = lax.axis_size("row")
    seqs, col_tok, feat = x.shape
    row_tok, _, pair_width = pair.shape
    width = wp.shape[1] // 2
    heads = score.shape[1]
    mixed = wv.shape[1]
    tokens = cols * col_tok
    per_col = col_tok // row_tok
    assert col_tok % row_tok == 0 and rows == per_col * cols and cols & (cols - 1) == 0
    assert heads * row_tok == 128 and 128 % width == 0 and width == col_tok
    mine = seqs * col_tok
    lanes = 2 * (row_tok + col_tok) * width

    swap = [
        (r * cols + c, (meet(r // per_col, c, cols) * per_col + r % per_col) * cols + r // per_col)
        for r in range(rows)
        for c in range(cols)
    ]
    xs = [lax.ppermute(x, "col", [(i, (i + k) % cols) for i in range(cols)]) for k in range(1, cols)]
    other_pair = lax.ppermute(pair, ("row", "col"), swap)

    (turn,) = call(turn_kernel, [((mine, mine), BF16)], [], flops=20_000_000_000, seqs=seqs, col_tok=col_tok)
    own, proj, w, token, seq, inv = call(
        own_kernel,
        [
            (x.shape, BF16), ((mine, 256), F32), ((feat, 256), BF16),
            ((tokens * width // 128, 128), F32), ((seqs, 128), F32), ((8, 128), F32),
        ],
        [x, wp, present, live, turn],
        flops=30_000_000, width=width,
    )
    send, xn = call(
        pack_kernel,
        [((rows, seqs, lanes), BF16), ((cols, seqs, col_tok, feat), BF16)],
        xs + [own, proj, w, turn, token, seq],
        cols=cols, rows=rows, col_tok=col_tok, row_tok=row_tok, width=width,
    )
    got = lax.all_to_all(send, "row", 0, 0)
    values, gate = call(
        values_kernel, [((seqs, tokens, mixed), BF16), ((mine, mixed), F32)], [xn, own, wv, wg], flops=100_000_000
    )
    pairs = row_tok * col_tok
    swap_matrix, state, other_state = call(
        order_kernel,
        [((pairs, pairs), BF16), ((pairs, pair_width), BF16), ((pairs, pair_width), BF16)],
        [pair, other_pair],
        flops=100_000_000,
    )
    sizes = dict(row_tok=row_tok, col_tok=col_tok, width=width)
    (chunk,) = call(
        score_kernel,
        [((rows, col_tok + 8, 128), BF16)],
        [got, other_state, mean, swap_matrix, score.T, inv],
        heads=heads, **sizes,
    )
    scores = lax.all_to_all(chunk, "row", 0, 0)
    (pair_new,) = call(
        transition_kernel,
        [(pair.shape, BF16)],
        [got, state, mean, swap_matrix, inv, win, wout],
        flops=1_000_000_000, **sizes,
    )
    alignment, pair_output = call(
        blend_kernel,
        [(x.shape, BF16), (pair.shape, BF16)],
        [scores, values, gate, x, wr.T, live.reshape(1, -1), pair_new],
        scratch=[pltpu.SemaphoreType.DMA], hbm_outs=1, cols=cols, per_col=per_col, row_tok=row_tok, col_tok=col_tok, heads=heads,
    )
    return alignment, pair_output


def solution(mesh):
    spread = P("row", "col", None)
    return jax.shard_map(
        body,
        mesh=mesh,
        in_specs=(spread, spread) + (P(),) * 10,
        out_specs=(spread, spread),
        check_vma=False,
    )
```
